256 devices in a mesh: ifg: 128 (over y, z_lo, x, core), slab: 2 (over z_hi).
Axes of the slice: x: 4, y: 4, z: 8 (z_hi: 2, z_lo: 4; z = z_hi * 4 + z_lo), core: 2. Of those that a mesh axis runs over, the one named last changes fastest.
Arguments:
- phase: float32 [2, 1152, 49152], P('slab', 'ifg'), may hold values from -60 to 60
- corrections: int32 [2, 1152, 49152], P('slab', 'ifg'), may hold values from -1 to 1
- closure_loops: int32 [288, 1152], replicated, may hold values from -1 to 1, as said below
- design: int32 [1152, 288], replicated, may hold values from -1 to 1, as said below
Outputs:
- closure_phase: float32 [2, 288, 49152], P('slab', None, 'ifg')
- displacement: float32 [2, 288, 49152], P('slab', None, 'ifg')
- misfit: float32 [2], P('slab')
The draws below stay inside these ranges and needn't reach their ends.
Inputs may be any that keep to these rules, and one draw needn't show every extreme that they name: Each row of closure_loops holds +1 at two interferograms and -1 at a third; closure_loops times design is zero. Each row of design holds one +1 and one -1 in different columns; every date is named by some row.
All inputs are finite; a program needn't handle non-finite values.
Results may differ from the reference program's by a relative error of at most 0.0003.
Values sent between devices are 32-bit elements; how exact they have to be, the bound alone decides.
No kernel may reach another device: no remote copies, remote signals or barrier semaphores. Data moves between devices by JAX's collectives and lax.ppermute only.
A program may use at most 64 MiB of HBM per device.

```python
import jax
import jax.numpy as jnp
from jax import lax

DATES = 288
IFGS = 1152
SLAB_PIX = 49152
SLABS = 2


two_pi = 6.283185307179586


def network(key):
    anchor = jnp.arange(DATES, dtype=jnp.int32)
    offsets = jax.random.randint(jax.random.fold_in(key, 11), (3, DATES), 1, 5)
    middle = (anchor + offsets[0]) % DATES
    finish = (anchor + offsets[0] + offsets[1]) % DATES
    spur_end = (anchor + offsets[2] + 4) % DATES
    start_dates = jnp.concatenate([anchor, middle, anchor, anchor])
    end_dates = jnp.concatenate([middle, finish, finish, spur_end])
    reorder = jax.random.permutation(jax.random.fold_in(key, 12), IFGS).astype(jnp.int32)
    columns = jnp.arange(DATES, dtype=jnp.int32)[None, :]
    design = (columns == end_dates[reorder][:, None]).astype(jnp.int32) - (columns == start_dates[reorder][:, None]).astype(jnp.int32)
    loop_ids = jnp.arange(DATES, dtype=jnp.int32)[:, None]
    source = reorder[None, :]
    closure = (source == loop_ids).astype(jnp.int32) + (source == loop_ids + DATES).astype(jnp.int32) - (source == loop_ids + 2 * DATES).astype(jnp.int32)
    return (closure, design)


def jump_counts(key):
    level = jax.random.randint(jax.random.fold_in(key, 21), (SLABS, IFGS, SLAB_PIX), 0, 10)
    return jnp.where(level == 0, -1, jnp.where(level == 9, 1, 0)).astype(jnp.int32)


def draw_closure_loops(key, part):
    return network(jax.random.fold_in(key, 5))[0]


def draw_design(key, part):
    return network(jax.random.fold_in(key, 5))[1]


def draw_corrections(key, part):
    return jump_counts(jax.random.fold_in(key, 6))


def draw_phase(key, part):
    closure, design = network(jax.random.fold_in(key, 5))
    design_float = design.astype(jnp.float32)
    counts = jump_counts(jax.random.fold_in(key, 6)).astype(jnp.float32)
    rising = 1.0 + 2.0 * jnp.arange(SLAB_PIX, dtype=jnp.float32) / SLAB_PIX
    epochs = jnp.arange(1, DATES + 1, dtype=jnp.float32) / DATES
    base = jax.random.fold_in(key, 31)
    slab_offset = 0.6 * jnp.arange(SLABS, dtype=jnp.float32) + 0.4 * jax.random.uniform(jax.random.fold_in(base, 4), (SLABS,), jnp.float32, 0.0, 1.0)
    rate = 0.5 * jnp.clip(jax.random.normal(jax.random.fold_in(base, 1), (SLABS, SLAB_PIX), jnp.float32), -4.0, 4.0) + 1.5 * rising[None, :] + slab_offset[:, None]
    weather = 0.5 * jnp.clip(jax.random.normal(jax.random.fold_in(base, 2), (SLABS, DATES, SLAB_PIX), jnp.float32), -4.0, 4.0)
    noise_part = 0.2 * rising[None, None, :] * jnp.clip(jax.random.normal(jax.random.fold_in(base, 3), (SLABS, IFGS, SLAB_PIX), jnp.float32), -4.0, 4.0)
    truth = 3.0 * rate[:, None, :] * epochs[None, :, None] + weather
    signal = jnp.einsum('md,sdp->smp', design_float, truth)
    return signal + noise_part - two_pi * counts


def setup_inputs(seed: int = 0) -> dict:
    arg_keys = jax.random.split(jax.random.key(seed), 5)
    phase = draw_phase(jax.random.fold_in(arg_keys[4], 71), 0)
    corrections = draw_corrections(jax.random.fold_in(arg_keys[4], 71), 0)
    closure_loops = draw_closure_loops(jax.random.fold_in(arg_keys[4], 71), 0)
    design = draw_design(jax.random.fold_in(arg_keys[4], 71), 0)
    return {"phase": phase, "corrections": corrections, "closure_loops": closure_loops, "design": design}


ridge_weight = 1.0
two_pi = 6.283185307179586
epsilon = 1e-06
highest = lax.Precision.HIGHEST

def reference(phase, corrections, closure_loops, design):
    loop_rows = closure_loops.astype(jnp.float32)
    design_float = design.astype(jnp.float32)
    normal = jnp.dot(design_float.T, design_float, precision=highest) + ridge_weight * jnp.eye(DATES, dtype=jnp.float32)

    def one_slab(members):
        phase_rows, counts = members
        corrected = phase_rows + two_pi * counts.astype(jnp.float32)
        closure = jnp.dot(loop_rows, corrected, precision=highest)
        projected = jnp.dot(design_float.T, corrected, precision=highest)
        shifts = jnp.linalg.solve(normal, projected)
        residual = corrected - jnp.dot(design_float, shifts, precision=highest)
        return (closure, shifts, jnp.sum(residual * residual))
    closure_phase, shifts, slab_square = lax.map(one_slab, (phase, corrections))
    frame_mean = lax.optimization_barrier(jnp.sum(shifts, axis=(0, 2))) / (SLABS * SLAB_PIX)
    displacement = shifts - frame_mean[None, :, None]
    misfit = jnp.sqrt(slab_square / (IFGS * SLAB_PIX) + epsilon)
    return (closure_phase, displacement, misfit)
```

```python
import functools

import jax
import jax.numpy as jnp
from jax import lax
from jax.experimental import pallas as pl
from jax.experimental.pallas import tpu as pltpu
from jax.sharding import Mesh
from jax.sharding import PartitionSpec as P

IFG = ("ifg_0", "ifg_1", "ifg_2", "ifg_3")
ALL = (*IFG, "slab")

ridge_weight = 1.0
two_pi = 6.283185307179586
epsilon = 1e-06
LANES = 128
VMEM = pl.BlockSpec(memory_space=pltpu.VMEM)
f32, bf16 = jnp.float32, jnp.bfloat16


def eye_mask(n):
    rows = lax.broadcasted_iota(jnp.int32, (n, n), 0)
    return rows == lax.broadcasted_iota(jnp.int32, (n, n), 1)


def head_kernel(parts, phase_ref, counts_ref, out_ref):
    rows, lines, _ = phase_ref.shape
    group = lines // parts
    for r in range(rows):
        for j in range(parts):
            at = pl.ds(j, group, stride=parts)
            out_ref[pl.ds(r * parts + j, group, stride=rows * parts), :] = phase_ref[
                r, at, :
            ] + two_pi * counts_ref[r, at, :].astype(f32)


def head(phase, counts, parts, steps):
    rows, lines, _ = phase.shape
    block = pl.BlockSpec((rows, lines // steps, LANES), lambda i: (0, i, 0))
    return pl.pallas_call(
        functools.partial(head_kernel, parts),
        grid=(steps,),
        in_specs=[block, block],
        out_specs=pl.BlockSpec((rows * lines // steps, LANES), lambda i: (i, 0)),
        out_shape=jax.ShapeDtypeStruct((rows * lines, LANES), f32),
        name="head",
    )(phase, counts)


def thirds(x):
    a = x.astype(bf16)
    rest = x - a.astype(f32)
    b = rest.astype(bf16)
    return a, b, (rest - b.astype(f32)).astype(bf16)


def exact_dot(left16, pieces):
    return sum(jnp.dot(left16, p, preferred_element_type=f32) for p in reversed(pieces))


def full_dot(left, right):
    a, b = thirds(left), thirds(right)
    pairs = ((0, 2), (2, 0), (1, 1), (0, 1), (1, 0), (0, 0))
    return sum(jnp.dot(a[i], b[j], preferred_element_type=f32) for i, j in pairs)


def prep_kernel(loops_ref, turned_ref, loops16_ref, design16_ref, turned16_ref, inverse_ref, power_ref):
    loops16_ref[...] = loops_ref[...].astype(f32).astype(bf16)
    turned = turned_ref[...].astype(f32)
    design16_ref[...] = turned.T.astype(bf16)
    turned16_ref[...] = turned.astype(bf16)
    eye = eye_mask(turned.shape[0])
    gram = jnp.dot(turned16_ref[...], design16_ref[...], preferred_element_type=f32)
    on_diagonal = jnp.where(eye, gram + ridge_weight, 0.0)
    column = jnp.sum(on_diagonal, axis=1, keepdims=True)
    row = jnp.sum(on_diagonal, axis=0, keepdims=True)
    step = jnp.where(eye, 0.0, -gram) / column
    power_ref[...] = step
    inverse_ref[...] = jnp.where(eye, 1.0, 0.0) + step

    def norm():
        return jnp.max(jnp.sum(power_ref[...], axis=1))

    def double(_):
        power = power_ref[...]
        power_ref[...] = full_dot(power, power)
        inverse_ref[...] += full_dot(inverse_ref[...], power_ref[...])
        return norm()

    lax.while_loop(lambda size: size > 1e-9, double, norm())
    inverse_ref[...] = inverse_ref[...] / row


def prep(loops, design):
    n, m = loops.shape
    dates = design.shape[1]
    return pl.pallas_call(
        prep_kernel,
        in_specs=[VMEM, VMEM],
        out_specs=[VMEM] * 4,
        out_shape=[
            jax.ShapeDtypeStruct((n, m), bf16),
            jax.ShapeDtypeStruct((m, dates), bf16),
            jax.ShapeDtypeStruct((dates, m), bf16),
            jax.ShapeDtypeStruct((dates, dates), f32),
        ],
        scratch_shapes=[pltpu.VMEM((dates, dates), f32)],
        name="prep",
    )(loops, design.T)


def copies_of(source_ref, held_ref, sems, chunks):
    rows = source_ref.shape[0] // chunks
    return [
        pltpu.make_async_copy(
            source_ref.at[pl.ds(k * rows, rows), :], held_ref.at[pl.ds(k * rows, rows), :], sems.at[k]
        )
        for k in range(chunks)
    ]


def side_by_side(held_ref, start, count, parts):
    return jnp.concatenate(
        [held_ref[pl.ds(start * parts + j, count, stride=parts), :] for j in range(parts)], axis=1
    )


def dates_kernel(parts, chunks, c_ref, design_ref, turned_ref, inverse_ref, shifts_ref, sums_ref, held_ref, sems):
    copies = copies_of(c_ref, held_ref, sems, chunks)
    for copy in copies:
        copy.start()
    ifgs, dates = design_ref.shape
    step = ifgs // chunks
    projected = 0.0
    for k in range(chunks):
        copies[k].wait()
        pieces = thirds(side_by_side(held_ref, k * step, step, parts))
        projected += exact_dot(turned_ref[:, k * step : (k + 1) * step], pieces)
    shifts = full_dot(inverse_ref[...], projected)
    shifts_ref[...] = shifts
    pieces = thirds(shifts)
    square = 0.0
    for k in range(chunks):
        model = exact_dot(design_ref[k * step : (k + 1) * step, :], pieces)
        residual = side_by_side(held_ref, k * step, step, parts) - model
        square += jnp.sum(residual * residual)
    ones = jnp.ones((8, shifts.shape[1]), bf16)
    sums_ref[:, :dates] = sum(
        lax.dot_general(ones, p, (((1,), (1,)), ((), ())), preferred_element_type=f32) for p in reversed(pieces)
    )
    sums_ref[:, dates:] = jnp.full((8, sums_ref.shape[1] - dates), square, f32)


def dates_part(c, design16, turned16, inverse, parts, width, chunks):
    dates = design16.shape[1]
    return pl.pallas_call(
        functools.partial(dates_kernel, parts, chunks),
        in_specs=[pl.BlockSpec(memory_space=pl.ANY)] + [VMEM] * 3,
        out_specs=[VMEM] * 2,
        out_shape=[
            jax.ShapeDtypeStruct((dates, parts * LANES), f32),
            jax.ShapeDtypeStruct((8, width), f32),
        ],
        scratch_shapes=[pltpu.VMEM(c.shape, f32), pltpu.SemaphoreType.DMA((chunks,))],
        name="dates",
    )(c, design16, turned16, inverse)


def loops_kernel(parts, chunks, c_ref, loops_ref, closure_ref, held_ref, sems):
    copies = copies_of(c_ref, held_ref, sems, chunks)
    for copy in copies:
        copy.start()
    step = loops_ref.shape[1] // chunks
    closure = 0.0
    for k in range(chunks):
        copies[k].wait()
        pieces = thirds(side_by_side(held_ref, k * step, step, parts))
        closure += exact_dot(loops_ref[:, k * step : (k + 1) * step], pieces)
    closure_ref[0] = closure


def loops_part(c, loops16, parts, chunks):
    return pl.pallas_call(
        functools.partial(loops_kernel, parts, chunks),
        in_specs=[pl.BlockSpec(memory_space=pl.ANY), VMEM],
        out_specs=VMEM,
        out_shape=jax.ShapeDtypeStruct((1, loops16.shape[0], parts * LANES), f32),
        scratch_shapes=[pltpu.VMEM(c.shape, f32), pltpu.SemaphoreType.DMA((chunks,))],
        name="loops",
    )(c, loops16)


def final_kernel(slabs, pixels, count, slab_ref, got_ref, shifts_ref, displacement_ref, misfit_ref):
    dates = displacement_ref.shape[1]
    got = got_ref[...]
    peers, width = got.shape
    total = jnp.sum(got[:, :dates], axis=0, keepdims=True) / (slabs * pixels)
    mine = lax.rem(lax.broadcasted_iota(jnp.int32, (peers, width - dates), 0), slabs) == slab_ref[0]
    square = jnp.sum(jnp.where(mine, got[:, dates:], 0.0), axis=0, keepdims=True)
    misfit_ref[...] = jnp.sqrt(square / count + epsilon)
    mean = jnp.sum(jnp.where(eye_mask(dates), total, 0.0), axis=1, keepdims=True)
    displacement_ref[0] = shifts_ref[...] - mean


def local(phase, corrections, closure_loops, design):
    slabs = lax.axis_size("slab")
    peers = lax.axis_size(IFG)
    rows, pixels = phase.shape[1:]
    parts = pixels // (peers * LANES)
    dates = design.shape[1]
    width = -(-(dates + 1) // LANES) * LANES
    lines = (rows, pixels // LANES, LANES)
    tiles = head(phase.reshape(lines), corrections.reshape(lines), parts, 8)
    got = lax.all_to_all(tiles.reshape(peers, 1, -1), IFG, split_axis=0, concat_axis=0, tiled=True)
    got = got.reshape(tiles.shape)
    loops16, design16, turned16, inverse = prep(closure_loops, design)
    shifts, sums = dates_part(got, design16, turned16, inverse, parts, width, 4)
    everyone = jnp.broadcast_to(sums[:1], (peers * slabs, 1, width))
    everyone = lax.all_to_all(everyone, ALL, split_axis=0, concat_axis=0, tiled=True)
    everyone = everyone.reshape(peers * slabs, width)
    closure = loops_part(got, loops16, parts, 4)
    displacement, misfit = pl.pallas_call(
        functools.partial(final_kernel, slabs, pixels, design.shape[0] * pixels),
        in_specs=[pl.BlockSpec(memory_space=pltpu.SMEM)] + [VMEM] * 2,
        out_specs=[VMEM] * 2,
        out_shape=[jax.ShapeDtypeStruct((1, dates, parts * LANES), f32), jax.ShapeDtypeStruct((1, width - dates), f32)],
        name="final",
    )(lax.axis_index("slab").reshape(1), everyone, shifts)
    return (closure, displacement, misfit[0, :1])


def solution(mesh):
    split = Mesh(
        mesh.devices.reshape(4, 4, 4, 2, mesh.shape["slab"]),
        (*IFG, "slab"),
    )
    in_specs = (P("slab", IFG, None), P("slab", IFG, None), P(), P())
    out_specs = (P("slab", None, IFG), P("slab", None, IFG), P("slab"))
    return jax.shard_map(local, mesh=split, in_specs=in_specs, out_specs=out_specs, check_vma=False)
```

```python
import functools

import jax
import jax.numpy as jnp
from jax import lax
from jax.experimental import pallas as pl
from jax.experimental.pallas import tpu as pltpu
from jax.sharding import Mesh
from jax.sharding import PartitionSpec as P

IFG = ("ifg_0", "ifg_1", "ifg_2", "ifg_3")

ridge_weight = 1.0
two_pi = 6.283185307179586
epsilon = 1e-06
LANES = 128
VMEM = pl.BlockSpec(memory_space=pltpu.VMEM)
ANY = pl.BlockSpec(memory_space=pl.ANY)
f32, bf16 = jnp.float32, jnp.bfloat16
PREP_VMEM = 66 * 1000 * 1000


def thirds(x):
    a = x.astype(bf16)
    rest = x - a.astype(f32)
    b = rest.astype(bf16)
    return a, b, (rest - b.astype(f32)).astype(bf16)


def exact_dot(left16, pieces):
    return sum(jnp.dot(left16, p, preferred_element_type=f32) for p in reversed(pieces))


def full_dot(left, right):
    a, b = thirds(left), thirds(right)
    pairs = ((0, 2), (2, 0), (1, 1), (0, 1), (1, 0), (0, 0))
    return sum(jnp.dot(a[i], b[j], preferred_element_type=f32) for i, j in pairs)


def head_kernel(parts, chunks, phase_ref, counts_ref, out_ref, phase_in, counts_in, sems):
    rows, lines, _ = phase_ref.shape
    peers = lines // parts
    span, group = lines // chunks, peers // chunks
    pitch = rows * parts + 1
    copies = []
    for k in range(chunks):
        at = pl.ds(k * span, span)
        for s, (a, b) in enumerate(((phase_ref, phase_in), (counts_ref, counts_in))):
            copies.append(pltpu.make_async_copy(a.at[:, at, :], b.at[:, at, :], sems.at[k, s]))
            copies[-1].start()
    sums = [jnp.zeros((8, LANES), f32) for _ in range(rows)]
    for k in range(chunks):
        copies[2 * k].wait()
        copies[2 * k + 1].wait()
        for r in range(rows):
            for j in range(parts):
                at = pl.ds(k * span + j, group, stride=parts)
                lines_in = phase_in[r, at, :] + two_pi * counts_in[r, at, :].astype(f32)
                out_ref[pl.ds(k * group * pitch + r * parts + j, group, stride=pitch), :] = lines_in
                sums[r] += jnp.sum(lines_in.reshape(group // 8, 8, LANES), axis=0)
    lane = lax.broadcasted_iota(jnp.int32, (1, LANES), 1)
    total = jnp.zeros((1, LANES), f32)
    for r in range(rows):
        total = jnp.where(lane == r, jnp.sum(sums[r], keepdims=True), total)
    out_ref[pl.ds(pitch - 1, peers, stride=pitch), :] = jnp.broadcast_to(total, (peers, LANES))


def head(phase, counts, parts, chunks):
    rows, lines, _ = phase.shape
    return pl.pallas_call(
        functools.partial(head_kernel, parts, chunks),
        in_specs=[ANY, ANY],
        out_specs=VMEM,
        out_shape=jax.ShapeDtypeStruct((lines // parts * (rows * parts + 1), LANES), f32),
        scratch_shapes=[
            pltpu.VMEM(phase.shape, f32),
            pltpu.VMEM(phase.shape, jnp.int32),
            pltpu.SemaphoreType.DMA((chunks, 2)),
        ],
        name="head",
    )(phase, counts)


def eye_mask(n):
    rows = lax.broadcasted_iota(jnp.int32, (n, n), 0)
    return rows == lax.broadcasted_iota(jnp.int32, (n, n), 1)


def prep_kernel(rows, loops_ref, turned_ref, loops16_ref, design16_ref, turned16_ref, inverse_ref, power_ref, tall_ref):
    ifgs = tall_ref.shape[0]
    peers = ifgs // rows
    for source, wide, tall in ((loops_ref, loops16_ref, None), (turned_ref, turned16_ref, design16_ref)):
        for start in range(0, source.shape[0], LANES):
            size = min(LANES, source.shape[0] - start)
            tall_ref[:, :size] = source[start : start + size, :].astype(f32).T
            for r in range(rows):
                some = tall_ref[pl.ds(r, peers, stride=rows), :]
                wide[start : start + size, r * peers : (r + 1) * peers] = some.T[:size].astype(bf16)
                if tall is not None:
                    tall[r * peers : (r + 1) * peers, start : start + size] = some[:, :size].astype(bf16)
    eye = eye_mask(turned_ref.shape[0])
    gram = jnp.dot(turned16_ref[...], design16_ref[...], preferred_element_type=f32)
    on_diagonal = jnp.where(eye, gram + ridge_weight, 0.0)
    column = jnp.sum(on_diagonal, axis=1, keepdims=True)
    row = jnp.sum(on_diagonal, axis=0, keepdims=True)
    step = jnp.where(eye, 0.0, -gram) / column
    power_ref[...] = step
    inverse_ref[...] = jnp.where(eye, 1.0, 0.0) + step

    def norm():
        return jnp.max(jnp.sum(power_ref[...], axis=1))

    def double(_):
        power = power_ref[...]
        power_ref[...] = full_dot(power, power)
        inverse_ref[...] += full_dot(inverse_ref[...], power_ref[...])
        return norm()

    lax.while_loop(lambda size: size > 1e-9, double, norm())
    inverse_ref[...] = inverse_ref[...] / row


def prep(loops, design, rows):
    n, m = loops.shape
    dates = design.shape[1]
    return pl.pallas_call(
        functools.partial(prep_kernel, rows),
        in_specs=[VMEM, VMEM],
        out_specs=[VMEM] * 4,
        out_shape=[
            jax.ShapeDtypeStruct((n, m), bf16),
            jax.ShapeDtypeStruct((m, dates), bf16),
            jax.ShapeDtypeStruct((dates, m), bf16),
            jax.ShapeDtypeStruct((dates, dates), f32),
        ],
        scratch_shapes=[pltpu.VMEM((dates, dates), f32), pltpu.VMEM((m, LANES), f32)],
        compiler_params=pltpu.CompilerParams(vmem_limit_bytes=PREP_VMEM),
        name="prep",
    )(loops, design.T)


def copies_of(source_ref, held_ref, sems, chunks):
    rows = source_ref.shape[0] // chunks
    return [
        pltpu.make_async_copy(
            source_ref.at[pl.ds(k * rows, rows), :], held_ref.at[pl.ds(k * rows, rows), :], sems.at[k]
        )
        for k in range(chunks)
    ]


def fetch(source_ref, held_ref, sems, chunks):
    copies = copies_of(source_ref, held_ref, sems, chunks)
    for copy in copies:
        copy.start()
    for copy in copies:
        copy.wait()


def lines_of(held_ref, r, parts, peers):
    pitch = held_ref.shape[0] // peers
    return jnp.concatenate(
        [held_ref[pl.ds(r * parts + j, peers, stride=pitch), :] for j in range(parts)], axis=1
    )


def dates_kernel(
    parts, rows, peers, chunks, c_ref, design_ref, turned_ref, inverse_ref, shifts_ref, square_ref, sums_ref, held_ref, sems
):
    fetch(c_ref, held_ref, sems, chunks)
    projected = 0.0
    for r in range(rows):
        pieces = thirds(lines_of(held_ref, r, parts, peers))
        projected += exact_dot(turned_ref[:, r * peers : (r + 1) * peers], pieces)
    shifts = full_dot(inverse_ref[...], projected)
    shifts_ref[...] = shifts
    pieces = thirds(shifts)[:2]
    square = 0.0
    for r in range(rows):
        model = exact_dot(design_ref[r * peers : (r + 1) * peers, :], pieces)
        residual = lines_of(held_ref, r, parts, peers) - model
        square += jnp.sum((residual * residual).reshape(peers // 8, 8, parts * LANES), axis=0)
    square_ref[...] = jnp.broadcast_to(jnp.sum(square, keepdims=True), square_ref.shape)
    pitch = held_ref.shape[0] // peers
    sums_ref[...] = held_ref[pl.ds(pitch - 1, peers, stride=pitch), :]


def dates_part(c, design16, turned16, inverse, parts, rows, peers, chunks):
    dates = design16.shape[1]
    return pl.pallas_call(
        functools.partial(dates_kernel, parts, rows, peers, chunks),
        in_specs=[ANY] + [VMEM] * 3,
        out_specs=[VMEM] * 3,
        out_shape=[
            jax.ShapeDtypeStruct((dates, parts * LANES), f32),
            jax.ShapeDtypeStruct((peers, LANES), f32),
            jax.ShapeDtypeStruct((peers, LANES), f32),
        ],
        scratch_shapes=[pltpu.VMEM(c.shape, f32), pltpu.SemaphoreType.DMA((chunks,))],
        name="dates",
    )(c, design16, turned16, inverse)


def loops_kernel(parts, rows, peers, chunks, c_ref, loops_ref, closure_ref, held_ref, sems):
    fetch(c_ref, held_ref, sems, chunks)
    closure = 0.0
    for r in range(rows):
        pieces = thirds(lines_of(held_ref, r, parts, peers))
        closure += exact_dot(loops_ref[:, r * peers : (r + 1) * peers], pieces)
    closure_ref[0] = closure


def loops_part(c, loops16, parts, rows, peers, chunks):
    return pl.pallas_call(
        functools.partial(loops_kernel, parts, rows, peers, chunks),
        in_specs=[ANY, VMEM],
        out_specs=VMEM,
        out_shape=jax.ShapeDtypeStruct((1, loops16.shape[0], parts * LANES), f32),
        scratch_shapes=[pltpu.VMEM(c.shape, f32), pltpu.SemaphoreType.DMA((chunks,))],
        name="loops",
    )(c, loops16)


def mean_kernel(rows, count, mine_ref, other_ref, turned_ref, inverse_ref, shifts_ref, displacement_ref):
    peers = mine_ref.shape[0]
    total = mine_ref[...] + other_ref[...]
    projected = 0.0
    for r in range(rows):
        column = jnp.broadcast_to(total[:, r : r + 1], (peers, LANES))
        projected += exact_dot(turned_ref[:, r * peers : (r + 1) * peers], thirds(column))
    mean = full_dot(inverse_ref[...], projected) / count
    for j in range(shifts_ref.shape[1] // LANES):
        at = slice(j * LANES, (j + 1) * LANES)
        displacement_ref[0, :, at] = shifts_ref[:, at] - mean


def mean_part(mine, other, turned16, inverse, shifts, rows, count):
    return pl.pallas_call(
        functools.partial(mean_kernel, rows, count),
        in_specs=[VMEM] * 5,
        out_specs=VMEM,
        out_shape=jax.ShapeDtypeStruct((1, *shifts.shape), f32),
        name="mean",
    )(mine, other, turned16, inverse, shifts)


def local(phase, corrections, closure_loops, design):
    slabs = lax.axis_size("slab")
    peers = lax.axis_size(IFG)
    rows, pixels = phase.shape[1:]
    parts = pixels // (peers * LANES)
    lines = (rows, pixels // LANES, LANES)
    tiles = head(phase.reshape(lines), corrections.reshape(lines), parts, 4)
    got = lax.all_to_all(tiles.reshape(peers, 1, -1), IFG, split_axis=0, concat_axis=0, tiled=True)
    got = got.reshape(tiles.shape)
    loops16, design16, turned16, inverse = prep(closure_loops, design, rows)
    shifts, square, sums = dates_part(got, design16, turned16, inverse, parts, rows, peers, 4)
    squares = lax.all_to_all(
        square.reshape(peers, 1, LANES), IFG, split_axis=0, concat_axis=0, tiled=True
    )
    other = lax.ppermute(sums, "slab", [(i, (i + 1) % slabs) for i in range(slabs)])
    closure = loops_part(got, loops16, parts, rows, peers, 4)
    displacement = mean_part(sums, other, turned16, inverse, shifts, rows, slabs * pixels)
    slab_square = jnp.sum(squares, axis=0)[0, :1]
    misfit = jnp.sqrt(slab_square / (design.shape[0] * pixels) + epsilon)
    return (closure, displacement, misfit)


def solution(mesh):
    split = Mesh(
        mesh.devices.reshape(4, 4, 4, 2, mesh.shape["slab"]),
        (*IFG, "slab"),
    )
    in_specs = (P("slab", IFG, None), P("slab", IFG, None), P(), P())
    out_specs = (P("slab", None, IFG), P("slab", None, IFG), P("slab"))
    return jax.shard_map(local, mesh=split, in_specs=in_specs, out_specs=out_specs, check_vma=False)
```

```python
import functools

import jax
import jax.numpy as jnp
from jax import lax
from jax.experimental import pallas as pl
from jax.experimental.pallas import tpu as pltpu
from jax.sharding import Mesh
from jax.sharding import PartitionSpec as P


IFG = ("ifg_0", "ifg_1", "ifg_2", "ifg_3")

ridge_weight = 1.0
two_pi = 6.283185307179586
epsilon = 1e-06
LANES = 128
VMEM = pl.BlockSpec(memory_space=pltpu.VMEM)
HBM = pl.BlockSpec(memory_space=pltpu.HBM)
SMEM = pl.BlockSpec(memory_space=pltpu.SMEM)
f32, bf16 = jnp.float32, jnp.bfloat16
SMALL = pltpu.CompilerParams(vmem_limit_bytes=16 * 2**20)


def in_hbm(x):
    return pltpu.with_memory_space_constraint(x, pltpu.HBM)


def thirds(x):
    a = x.astype(bf16)
    rest = x - a.astype(f32)
    b = rest.astype(bf16)
    return a, b, (rest - b.astype(f32)).astype(bf16)


PAIRS = ((0, 0), (0, 1), (0, 2), (1, 0), (1, 1), (2, 0))


def stack_right(stack_ref, x):
    pieces = thirds(x)
    n = x.shape[0]
    for k, (_, j) in enumerate(PAIRS):
        stack_ref[k * n : (k + 1) * n, :] = pieces[j]


def side_by_side(wide_ref, at, x):
    n = x.shape[1]
    for k, piece in enumerate(thirds(x)):
        wide_ref[at, k * n : (k + 1) * n] = piece


def folded(wide, count):
    n = wide.shape[1] // count
    return sum(wide[:, k * n : (k + 1) * n] for k in reversed(range(count)))


def head_kernel(parts, chunks, phase_ref, counts_ref, out_ref, sums_ref, phase_in, counts_in, sems):
    rows, lines, _ = phase_ref.shape
    peers = lines // parts
    span, group = lines // chunks, peers // chunks
    pitch = rows * parts
    copies = []
    for k in range(chunks):
        at = pl.ds(k * span, span)
        for s, (a, b) in enumerate(((phase_ref, phase_in), (counts_ref, counts_in))):
            copies.append(pltpu.make_async_copy(a.at[:, at, :], b.at[:, at, :], sems.at[k, s]))
            copies[-1].start()
    sums = [jnp.zeros((8, LANES), f32) for _ in range(rows)]
    for k in range(chunks):
        copies[2 * k].wait()
        copies[2 * k + 1].wait()
        for r in range(rows):
            for j in range(parts):
                at = pl.ds(k * span + j, group, stride=parts)
                some = phase_in[r, at, :] + two_pi * counts_in[r, at, :].astype(f32)
                out_ref[pl.ds(k * group * pitch + r * parts + j, group, stride=pitch), :] = some
                sums[r] += jnp.sum(some.reshape(group // 8, 8, LANES), axis=0)
    lane = lax.broadcasted_iota(jnp.int32, (1, LANES), 1)
    total = jnp.zeros((1, LANES), f32)
    for r in range(rows):
        total = jnp.where(lane == r + 1, jnp.sum(sums[r], keepdims=True), total)
    sums_ref[...] = jnp.broadcast_to(total, sums_ref.shape)


def head(phase, counts, parts, chunks):
    rows, lines, _ = phase.shape
    return pl.pallas_call(
        functools.partial(head_kernel, parts, chunks),
        in_specs=[HBM, HBM],
        out_specs=[VMEM, VMEM],
        out_shape=[pltpu.HBM((lines * rows, LANES), f32), jax.ShapeDtypeStruct((8, LANES), f32)],
        scratch_shapes=[
            pltpu.VMEM(phase.shape, f32),
            pltpu.VMEM(phase.shape, jnp.int32),
            pltpu.SemaphoreType.DMA((chunks, 2)),
        ],
        name="head",
    )(in_hbm(phase), in_hbm(counts))


def eye_mask(n):
    rows = lax.broadcasted_iota(jnp.int32, (n, n), 0)
    return rows == lax.broadcasted_iota(jnp.int32, (n, n), 1)


def doubled(left_ref, right_ref, power_ref, total_ref):
    n = power_ref.shape[0]
    power, total = power_ref[...], total_ref[...]
    stack_right(right_ref, power)
    for half, x in enumerate((power, total)):
        pieces = thirds(x)
        for k, (i, _) in enumerate(PAIRS):
            left_ref[half * n : (half + 1) * n, k * n : (k + 1) * n] = pieces[i]
    both = jnp.dot(left_ref[...], right_ref[...], preferred_element_type=f32)
    power_ref[...] = both[:n]
    total_ref[...] = total + both[n:]


def prep_kernel(
    rows, loops_ref, turned_ref, loops16_ref, design16_ref, turned16_ref, six_ref, direct_ref,
    tall_ref, power_ref, total_ref, left_ref, right_ref,
):
    peers = tall_ref.shape[0] // rows
    for source, wide, tall in ((loops_ref, loops16_ref, None), (turned_ref, turned16_ref, design16_ref)):
        for start in range(0, source.shape[0], LANES):
            size = min(LANES, source.shape[0] - start)
            tall_ref[:, :size] = source[start : start + size, :].astype(f32).T
            for r in range(rows):
                some = tall_ref[pl.ds(r, peers, stride=rows), :]
                wide[start : start + size, r * peers : (r + 1) * peers] = some.T[:size].astype(bf16)
                if tall is not None:
                    tall[r * peers : (r + 1) * peers, start : start + size] = some[:, :size].astype(bf16)
    eye = eye_mask(turned_ref.shape[0])
    gram = jnp.dot(turned16_ref[...], design16_ref[...], preferred_element_type=f32)
    on_diagonal = jnp.where(eye, gram + ridge_weight, 0.0)
    column = jnp.sum(on_diagonal, axis=1, keepdims=True)
    row = jnp.sum(on_diagonal, axis=0, keepdims=True)
    power_ref[...] = jnp.where(eye, 0.0, -gram) / column
    total_ref[...] = jnp.where(eye, 1.0, 0.0)

    def norm():
        return jnp.max(jnp.sum(power_ref[...], axis=1))

    def double(_):
        doubled(left_ref, right_ref, power_ref, total_ref)
        return norm()

    lax.while_loop(lambda size: size > 3e-8, double, norm())
    pieces = thirds(total_ref[...] / row)
    n = total_ref.shape[0]
    for k, (i, _) in enumerate(PAIRS):
        six_ref[:, k * n : (k + 1) * n] = pieces[i]
    direct_ref[...] = sum(jnp.dot(p, turned16_ref[...], preferred_element_type=f32) for p in reversed(pieces))


def prep(loops, design, rows):
    n, m = loops.shape
    dates = design.shape[1]
    return pl.pallas_call(
        functools.partial(prep_kernel, rows),
        in_specs=[VMEM, VMEM],
        out_specs=[VMEM] * 5,
        out_shape=[
            pltpu.HBM((n, m), bf16),
            pltpu.HBM((m, dates), bf16),
            pltpu.HBM((dates, m), bf16),
            pltpu.HBM((dates, dates * len(PAIRS)), bf16),
            pltpu.HBM((dates, m), f32),
        ],
        scratch_shapes=[
            pltpu.VMEM((m, LANES), f32),
            pltpu.VMEM((dates, dates), f32),
            pltpu.VMEM((dates, dates), f32),
            pltpu.VMEM((2 * dates, dates * len(PAIRS)), bf16),
            pltpu.VMEM((dates * len(PAIRS), dates), bf16),
        ],
        compiler_params=SMALL,
        name="prep",
    )(loops, design.T)


def lines_of(held_ref, r, parts, peers):
    pitch = held_ref.shape[0] // peers
    return jnp.concatenate(
        [held_ref[pl.ds(r * parts + j, peers, stride=pitch), :] for j in range(parts)], axis=1
    )


def dates_kernel(
    parts, rows, peers, held_ref, mine_ref, other_ref, turned_hbm, six_hbm, design_hbm, shifts_ref, line_ref,
    turned_ref, six_ref, design_ref, wide_ref, stack_ref, sems,
):
    copies = [
        pltpu.make_async_copy(turned_hbm, turned_ref, sems.at[0]),
        pltpu.make_async_copy(six_hbm, six_ref, sems.at[1]),
        pltpu.make_async_copy(design_hbm, design_ref, sems.at[2]),
    ]
    for copy in copies:
        copy.start()
    for r in range(rows):
        side_by_side(wide_ref, slice(r * peers, (r + 1) * peers), lines_of(held_ref, r, parts, peers))
    copies[0].wait()
    projected = folded(jnp.dot(turned_ref[...], wide_ref[...], preferred_element_type=f32), 3)
    stack_right(stack_ref, projected)
    copies[1].wait()
    shifts = jnp.dot(six_ref[...], stack_ref[...], preferred_element_type=f32)
    shifts_ref[...] = shifts
    two = jnp.concatenate(thirds(shifts)[:2], axis=1)
    copies[2].wait()
    square = 0.0
    for r in range(rows):
        model = folded(jnp.dot(design_ref[r * peers : (r + 1) * peers, :], two, preferred_element_type=f32), 2)
        residual = lines_of(held_ref, r, parts, peers) - model
        square += jnp.sum((residual * residual).reshape(peers // 8, 8, parts * LANES), axis=0)
    lane = lax.broadcasted_iota(jnp.int32, (1, LANES), 1)
    line = jnp.where(lane == 0, jnp.sum(square, keepdims=True), mine_ref[:1] + other_ref[:1])
    line_ref[...] = jnp.broadcast_to(line, line_ref.shape)


def dates_part(c, turned16, mine, other, design16, six, parts, rows, peers):
    ifgs, dates = design16.shape
    return pl.pallas_call(
        functools.partial(dates_kernel, parts, rows, peers),
        in_specs=[VMEM] * 3 + [HBM] * 3,
        out_specs=[VMEM] * 2,
        out_shape=[
            jax.ShapeDtypeStruct((dates, parts * LANES), f32),
            pltpu.HBM((peers, LANES), f32),
        ],
        scratch_shapes=[
            pltpu.VMEM(turned16.shape, bf16),
            pltpu.VMEM(six.shape, bf16),
            pltpu.VMEM(design16.shape, bf16),
            pltpu.VMEM((ifgs, 3 * parts * LANES), bf16),
            pltpu.VMEM((dates * len(PAIRS), parts * LANES), bf16),
            pltpu.SemaphoreType.DMA((3,)),
        ],
        compiler_params=SMALL,
        name="dates",
    )(c, mine, other, in_hbm(turned16), in_hbm(six), in_hbm(design16))


def loops_kernel(parts, rows, peers, held_ref, loops_hbm, closure_ref, loops_ref, wide_ref, sem):
    copy = pltpu.make_async_copy(loops_hbm, loops_ref, sem)
    copy.start()
    for r in range(rows):
        side_by_side(wide_ref, slice(r * peers, (r + 1) * peers), lines_of(held_ref, r, parts, peers))
    copy.wait()
    closure_ref[0] = folded(jnp.dot(loops_ref[...], wide_ref[...], preferred_element_type=f32), 3)


def loops_part(c, loops16, parts, rows, peers):
    return pl.pallas_call(
        functools.partial(loops_kernel, parts, rows, peers),
        in_specs=[VMEM, HBM],
        out_specs=VMEM,
        out_shape=jax.ShapeDtypeStruct((1, loops16.shape[0], parts * LANES), f32),
        scratch_shapes=[
            pltpu.VMEM(loops16.shape, bf16),
            pltpu.VMEM((loops16.shape[1], 3 * parts * LANES), bf16),
            pltpu.SemaphoreType.DMA,
        ],
        compiler_params=SMALL,
        name="loops",
    )(c, in_hbm(loops16))


def last_kernel(rows, count, squares, got_ref, direct_ref, shifts_ref, displacement_ref, misfit_ref):
    by_lane = got_ref[...].T
    square = jnp.sum(by_lane[:1], axis=1, keepdims=True)
    misfit_ref[...] = jnp.broadcast_to(jnp.sqrt(square / squares + epsilon), misfit_ref.shape)
    line = jnp.concatenate([by_lane[r + 1 : r + 2] for r in range(rows)], axis=1)
    mean = jnp.sum(direct_ref[...] * line, axis=1, keepdims=True) / count
    displacement_ref[0] = shifts_ref[...] - mean


def last_part(got, direct, shifts, rows, count, squares):
    return pl.pallas_call(
        functools.partial(last_kernel, rows, count, squares),
        in_specs=[VMEM] * 3,
        out_specs=[VMEM] * 2,
        out_shape=[
            jax.ShapeDtypeStruct((1, *shifts.shape), f32),
            jax.ShapeDtypeStruct((1, LANES), f32),
        ],
        compiler_params=SMALL,
        name="last",
    )(got, direct, shifts)


def local(phase, corrections, closure_loops, design):
    slabs = lax.axis_size("slab")
    peers = lax.axis_size(IFG)
    rows, pixels = phase.shape[1:]
    parts = pixels // (peers * LANES)
    lines = (rows, pixels // LANES, LANES)
    tiles, mine = head(phase.reshape(lines), corrections.reshape(lines), parts, 4)
    got = lax.all_to_all(tiles.reshape(peers, 1, -1), IFG, split_axis=0, concat_axis=0, tiled=True)
    got = got.reshape(tiles.shape)
    other = lax.ppermute(mine, "slab", [(i, (i + 1) % slabs) for i in range(slabs)])
    loops16, design16, turned16, six, direct = prep(closure_loops, design, rows)
    shifts, line = dates_part(got, turned16, mine, other, design16, six, parts, rows, peers)
    totals = lax.all_to_all(line.reshape(peers, 1, LANES), IFG, split_axis=0, concat_axis=0, tiled=True)
    closure = loops_part(got, loops16, parts, rows, peers)
    displacement, misfit = last_part(
        totals.reshape(peers, LANES), direct, shifts, rows, slabs * pixels, design.shape[0] * pixels
    )
    return (closure, displacement, misfit[0, :1])


def solution(mesh):
    split = Mesh(
        mesh.devices.reshape(4, 4, 4, 2, mesh.shape["slab"]),
        (*IFG, "slab"),
    )
    in_specs = (P("slab", IFG, None), P("slab", IFG, None), P(), P())
    out_specs = (P("slab", None, IFG), P("slab", None, IFG), P("slab"))
    return jax.shard_map(local, mesh=split, in_specs=in_specs, out_specs=out_specs, check_vma=False)
```

```python
import functools

import jax
import jax.numpy as jnp
from jax import lax
from jax.experimental import pallas as pl
from jax.experimental.pallas import tpu as pltpu
from jax.sharding import Mesh
from jax.sharding import PartitionSpec as P


IFG = ("ifg_0", "ifg_1", "ifg_2", "ifg_3")

ridge_weight = 1.0
two_pi = 6.283185307179586
epsilon = 1e-06
LANES = 128
VMEM = pl.BlockSpec(memory_space=pltpu.VMEM)
HBM = pl.BlockSpec(memory_space=pltpu.HBM)
SMEM = pl.BlockSpec(memory_space=pltpu.SMEM)
f32, bf16 = jnp.float32, jnp.bfloat16
SMALL = pltpu.CompilerParams(vmem_limit_bytes=16 * 2**20)


def in_hbm(x):
    return pltpu.with_memory_space_constraint(x, pltpu.HBM)


def thirds(x):
    a = x.astype(bf16)
    rest = x - a.astype(f32)
    b = rest.astype(bf16)
    return a, b, (rest - b.astype(f32)).astype(bf16)


PAIRS = ((0, 0), (0, 1), (0, 2), (1, 0), (1, 1), (2, 0))


def stack_right(stack_ref, x):
    pieces = thirds(x)
    n = x.shape[0]
    for k, (_, j) in enumerate(PAIRS):
        stack_ref[k * n : (k + 1) * n, :] = pieces[j]


def side_by_side(wide_ref, at, x):
    n = x.shape[1]
    for k, piece in enumerate(thirds(x)):
        wide_ref[at, k * n : (k + 1) * n] = piece


def folded(wide, count):
    n = wide.shape[1] // count
    return sum(wide[:, k * n : (k + 1) * n] for k in reversed(range(count)))


def head_kernel(parts, chunks, phase_ref, counts_ref, out_ref, sums_ref, phase_in, counts_in, sems):
    rows, lines, _ = phase_ref.shape
    peers = lines // parts
    span, group = lines // chunks, peers // chunks
    pitch = rows * parts
    copies = []
    for k in range(chunks):
        at = pl.ds(k * span, span)
        for s, (a, b) in enumerate(((phase_ref, phase_in), (counts_ref, counts_in))):
            copies.append(pltpu.make_async_copy(a.at[:, at, :], b.at[:, at, :], sems.at[k, s]))
            copies[-1].start()
    sums = [jnp.zeros((8, LANES), f32) for _ in range(rows)]
    for k in range(chunks):
        copies[2 * k].wait()
        copies[2 * k + 1].wait()
        for r in range(rows):
            for j in range(parts):
                at = pl.ds(k * span + j, group, stride=parts)
                some = phase_in[r, at, :] + two_pi * counts_in[r, at, :].astype(f32)
                out_ref[pl.ds(k * group * pitch + r * parts + j, group, stride=pitch), :] = some
                sums[r] += jnp.sum(some.reshape(group // 8, 8, LANES), axis=0)
    lane = lax.broadcasted_iota(jnp.int32, (1, LANES), 1)
    total = jnp.zeros((1, LANES), f32)
    for r in range(rows):
        total = jnp.where(lane == r + 1, jnp.sum(sums[r], keepdims=True), total)
    sums_ref[...] = jnp.broadcast_to(total, sums_ref.shape)


def head(phase, counts, parts, chunks):
    rows, lines, _ = phase.shape
    return pl.pallas_call(
        functools.partial(head_kernel, parts, chunks),
        in_specs=[HBM, HBM],
        out_specs=[VMEM, VMEM],
        out_shape=[pltpu.HBM((lines * rows, LANES), f32), jax.ShapeDtypeStruct((8, LANES), f32)],
        scratch_shapes=[
            pltpu.VMEM(phase.shape, f32),
            pltpu.VMEM(phase.shape, jnp.int32),
            pltpu.SemaphoreType.DMA((chunks, 2)),
        ],
        name="head",
    )(in_hbm(phase), in_hbm(counts))


def eye_mask(n):
    rows = lax.broadcasted_iota(jnp.int32, (n, n), 0)
    return rows == lax.broadcasted_iota(jnp.int32, (n, n), 1)


def doubled(left_ref, right_ref, power_ref, total_ref):
    n = power_ref.shape[0]
    power, total = power_ref[...], total_ref[...]
    stack_right(right_ref, power)
    for half, x in enumerate((power, total)):
        pieces = thirds(x)
        for k, (i, _) in enumerate(PAIRS):
            left_ref[half * n : (half + 1) * n, k * n : (k + 1) * n] = pieces[i]
    both = jnp.dot(left_ref[...], right_ref[...], preferred_element_type=f32)
    power_ref[...] = both[:n]
    total_ref[...] = total + both[n:]


def prep_kernel(
    rows, loops_ref, turned_ref, both16_ref, design16_ref, six_ref, direct_ref,
    tall_ref, power_ref, total_ref, left_ref, right_ref,
):
    peers = tall_ref.shape[0] // rows
    n = turned_ref.shape[0]
    for source, base, tall in ((loops_ref, n, None), (turned_ref, 0, design16_ref)):
        for start in range(0, source.shape[0], LANES):
            size = min(LANES, source.shape[0] - start)
            tall_ref[:, :size] = source[start : start + size, :].astype(f32).T
            for r in range(rows):
                some = tall_ref[pl.ds(r, peers, stride=rows), :]
                both16_ref[base + start : base + start + size, r * peers : (r + 1) * peers] = some.T[:size].astype(bf16)
                if tall is not None:
                    tall[r * peers : (r + 1) * peers, start : start + size] = some[:, :size].astype(bf16)
    eye = eye_mask(n)
    turned16 = both16_ref[:n, :]
    gram = jnp.dot(turned16, design16_ref[...], preferred_element_type=f32)
    on_diagonal = jnp.where(eye, gram + ridge_weight, 0.0)
    column = jnp.sum(on_diagonal, axis=1, keepdims=True)
    row = jnp.sum(on_diagonal, axis=0, keepdims=True)
    power_ref[...] = jnp.where(eye, 0.0, -gram) / column
    total_ref[...] = jnp.where(eye, 1.0, 0.0)

    def norm():
        return jnp.max(jnp.sum(power_ref[...], axis=1))

    def double(_):
        doubled(left_ref, right_ref, power_ref, total_ref)
        return norm()

    lax.while_loop(lambda size: size > 3e-8, double, norm())
    pieces = thirds(total_ref[...] / row)
    for k, (i, _) in enumerate(PAIRS):
        six_ref[:, k * n : (k + 1) * n] = pieces[i]
    direct_ref[...] = sum(jnp.dot(p, both16_ref[:n, :], preferred_element_type=f32) for p in reversed(pieces))


def prep(loops, design, rows):
    n, m = loops.shape
    dates = design.shape[1]
    return pl.pallas_call(
        functools.partial(prep_kernel, rows),
        in_specs=[VMEM, VMEM],
        out_specs=[VMEM] * 4,
        out_shape=[
            pltpu.HBM((dates + n, m), bf16),
            pltpu.HBM((m, dates), bf16),
            pltpu.HBM((dates, dates * len(PAIRS)), bf16),
            pltpu.HBM((dates, m), f32),
        ],
        scratch_shapes=[
            pltpu.VMEM((m, LANES), f32),
            pltpu.VMEM((dates, dates), f32),
            pltpu.VMEM((dates, dates), f32),
            pltpu.VMEM((2 * dates, dates * len(PAIRS)), bf16),
            pltpu.VMEM((dates * len(PAIRS), dates), bf16),
        ],
        compiler_params=SMALL,
        name="prep",
    )(loops, design.T)


def lines_of(held_ref, r, parts, peers):
    pitch = held_ref.shape[0] // peers
    return jnp.concatenate(
        [held_ref[pl.ds(r * parts + j, peers, stride=pitch), :] for j in range(parts)], axis=1
    )


def main_kernel(
    parts, rows, peers, held_ref, mine_ref, other_ref, both_hbm, six_hbm, design_hbm, shifts_ref, line_ref, closure_hbm,
    both_ref, six_ref, design_ref, wide_ref, stack_ref, closure_ref, sems,
):
    pairs = ((both_hbm, both_ref), (six_hbm, six_ref), (design_hbm, design_ref))
    copies = [pltpu.make_async_copy(a, b, sems.at[k]) for k, (a, b) in enumerate(pairs)]
    copies[0].start()
    for r in range(rows):
        side_by_side(wide_ref, slice(r * peers, (r + 1) * peers), lines_of(held_ref, r, parts, peers))
    copies[0].wait()
    copies[1].start()
    copies[2].start()
    products = folded(jnp.dot(both_ref[...], wide_ref[...], preferred_element_type=f32), 3)
    dates = shifts_ref.shape[0]
    closure_ref[...] = products[dates:]
    copies.append(pltpu.make_async_copy(closure_ref, closure_hbm.at[0], sems.at[3]))
    copies[3].start()
    stack_right(stack_ref, products[:dates])
    copies[1].wait()
    shifts = jnp.dot(six_ref[...], stack_ref[...], preferred_element_type=f32)
    shifts_ref[...] = shifts
    two = jnp.concatenate(thirds(shifts)[:2], axis=1)
    copies[2].wait()
    model = folded(jnp.dot(design_ref[...], two, preferred_element_type=f32), 2)
    square = 0.0
    for r in range(rows):
        residual = lines_of(held_ref, r, parts, peers) - model[r * peers : (r + 1) * peers]
        square += jnp.sum((residual * residual).reshape(peers // 8, 8, parts * LANES), axis=0)
    lane = lax.broadcasted_iota(jnp.int32, (1, LANES), 1)
    line = jnp.where(lane == 0, jnp.sum(square, keepdims=True), mine_ref[:1] + other_ref[:1])
    line_ref[...] = jnp.broadcast_to(line, line_ref.shape)
    copies[3].wait()


def main_part(c, mine, other, both16, six, design16, parts, rows, peers):
    ifgs, dates = design16.shape
    pixels = parts * LANES
    n = both16.shape[0] - dates
    return pl.pallas_call(
        functools.partial(main_kernel, parts, rows, peers),
        in_specs=[VMEM] * 3 + [HBM] * 3,
        out_specs=[VMEM, VMEM, HBM],
        out_shape=[
            jax.ShapeDtypeStruct((dates, pixels), f32),
            jax.ShapeDtypeStruct((peers, LANES), f32),
            pltpu.HBM((1, n, pixels), f32),
        ],
        scratch_shapes=[
            pltpu.VMEM(both16.shape, bf16),
            pltpu.VMEM(six.shape, bf16),
            pltpu.VMEM(design16.shape, bf16),
            pltpu.VMEM((ifgs, 3 * pixels), bf16),
            pltpu.VMEM((dates * len(PAIRS), pixels), bf16),
            pltpu.VMEM((n, pixels), f32),
            pltpu.SemaphoreType.DMA((4,)),
        ],
        compiler_params=pltpu.CompilerParams(vmem_limit_bytes=28 * 2**20),
        name="main",
    )(c, mine, other, in_hbm(both16), in_hbm(six), in_hbm(design16))


def last_kernel(rows, count, squares, got_ref, direct_ref, shifts_ref, displacement_ref, misfit_ref):
    by_lane = got_ref[...].T
    square = jnp.sum(by_lane[:1], axis=1, keepdims=True)
    misfit_ref[...] = jnp.broadcast_to(jnp.sqrt(square / squares + epsilon), misfit_ref.shape)
    line = jnp.concatenate([by_lane[r + 1 : r + 2] for r in range(rows)], axis=1)
    mean = jnp.sum(direct_ref[...] * line, axis=1, keepdims=True) / count
    displacement_ref[0] = shifts_ref[...] - mean


def last_part(got, direct, shifts, rows, count, squares):
    return pl.pallas_call(
        functools.partial(last_kernel, rows, count, squares),
        in_specs=[VMEM] * 3,
        out_specs=[VMEM] * 2,
        out_shape=[
            jax.ShapeDtypeStruct((1, *shifts.shape), f32),
            jax.ShapeDtypeStruct((1, LANES), f32),
        ],
        compiler_params=SMALL,
        name="last",
    )(got, direct, shifts)


def local(phase, corrections, closure_loops, design):
    slabs = lax.axis_size("slab")
    peers = lax.axis_size(IFG)
    rows, pixels = phase.shape[1:]
    parts = pixels // (peers * LANES)
    lines = (rows, pixels // LANES, LANES)
    tiles, mine = head(phase.reshape(lines), corrections.reshape(lines), parts, 4)
    got = lax.all_to_all(tiles.reshape(peers, 1, -1), IFG, split_axis=0, concat_axis=0, tiled=True)
    got = got.reshape(tiles.shape)
    other = lax.ppermute(mine, "slab", [(i, (i + 1) % slabs) for i in range(slabs)])
    both16, design16, six, direct = prep(closure_loops, design, rows)
    shifts, line, closure = main_part(got, mine, other, both16, six, design16, parts, rows, peers)
    totals = lax.all_to_all(line.reshape(peers, 1, LANES), IFG, split_axis=0, concat_axis=0, tiled=True)
    displacement, misfit = last_part(
        totals.reshape(peers, LANES), direct, shifts, rows, slabs * pixels, design.shape[0] * pixels
    )
    return (closure, displacement, misfit[0, :1])


def solution(mesh):
    split = Mesh(
        mesh.devices.reshape(4, 4, 4, 2, mesh.shape["slab"]),
        (*IFG, "slab"),
    )
    in_specs = (P("slab", IFG, None), P("slab", IFG, None), P(), P())
    out_specs = (P("slab", None, IFG), P("slab", None, IFG), P("slab"))
    return jax.shard_map(local, mesh=split, in_specs=in_specs, out_specs=out_specs, check_vma=False)
```

```python
import functools

import jax
import jax.numpy as jnp
from jax import lax
from jax.experimental import pallas as pl
from jax.experimental.pallas import tpu as pltpu
from jax.sharding import Mesh
from jax.sharding import PartitionSpec as P


IFG = ("ifg_0", "ifg_1", "ifg_2", "ifg_3")

ridge_weight = 1.0
two_pi = 6.283185307179586
epsilon = 1e-06
LANES = 128
VMEM = pl.BlockSpec(memory_space=pltpu.VMEM)
HBM = pl.BlockSpec(memory_space=pltpu.HBM)
SMEM = pl.BlockSpec(memory_space=pltpu.SMEM)
f32, bf16 = jnp.float32, jnp.bfloat16
SMALL = pltpu.CompilerParams(vmem_limit_bytes=16 * 2**20)


def in_hbm(x):
    return pltpu.with_memory_space_constraint(x, pltpu.HBM)


def thirds(x):
    a = x.astype(bf16)
    rest = x - a.astype(f32)
    b = rest.astype(bf16)
    return a, b, (rest - b.astype(f32)).astype(bf16)


PAIRS = ((0, 0), (0, 1), (0, 2), (1, 0), (1, 1), (2, 0))


def stack_right(stack_ref, x):
    pieces = thirds(x)
    n = x.shape[0]
    for k, (_, j) in enumerate(PAIRS):
        stack_ref[k * n : (k + 1) * n, :] = pieces[j]


def side_by_side(wide_ref, at, x):
    n = x.shape[1]
    for k, piece in enumerate(thirds(x)):
        wide_ref[at, k * n : (k + 1) * n] = piece


def folded(wide, count):
    n = wide.shape[1] // count
    return sum(wide[:, k * n : (k + 1) * n] for k in reversed(range(count)))


def head_kernel(parts, chunks, phase_ref, counts_ref, out_ref, phase_in, counts_in, sems):
    rows, lines, _ = phase_ref.shape
    peers = lines // parts
    span, group = lines // chunks, peers // chunks
    pitch = rows * parts
    copies = []
    for k in range(chunks):
        at = pl.ds(k * span, span)
        for s, (a, b) in enumerate(((phase_ref, phase_in), (counts_ref, counts_in))):
            copies.append(pltpu.make_async_copy(a.at[:, at, :], b.at[:, at, :], sems.at[k, s]))
            copies[-1].start()
    for k in range(chunks):
        copies[2 * k].wait()
        copies[2 * k + 1].wait()
        for r in range(rows):
            for j in range(parts):
                at = pl.ds(k * span + j, group, stride=parts)
                some = phase_in[r, at, :] + two_pi * counts_in[r, at, :].astype(f32)
                out_ref[pl.ds(k * group * pitch + r * parts + j, group, stride=pitch), :] = some


def head(phase, counts, parts, chunks):
    rows, lines, _ = phase.shape
    return pl.pallas_call(
        functools.partial(head_kernel, parts, chunks),
        in_specs=[HBM, HBM],
        out_specs=VMEM,
        out_shape=pltpu.HBM((lines * rows, LANES), f32),
        scratch_shapes=[
            pltpu.VMEM(phase.shape, f32),
            pltpu.VMEM(phase.shape, jnp.int32),
            pltpu.SemaphoreType.DMA((chunks, 2)),
        ],
        name="head",
    )(in_hbm(phase), in_hbm(counts))


def sums_kernel(rows, parts, peers, tiles_ref, sums_ref):
    pitch = rows * parts
    lane = lax.broadcasted_iota(jnp.int32, (1, LANES), 1)
    total = jnp.zeros((1, LANES), f32)
    for r in range(rows):
        row = 0.0
        for j in range(parts):
            some = tiles_ref[pl.ds(r * parts + j, peers, stride=pitch), :]
            row += jnp.sum(some.reshape(peers // 8, 8, LANES), axis=0)
        total = jnp.where(lane == r + 1, jnp.sum(row, keepdims=True), total)
    sums_ref[...] = jnp.broadcast_to(total, sums_ref.shape)


def sums_part(tiles, rows, parts, peers):
    return pl.pallas_call(
        functools.partial(sums_kernel, rows, parts, peers),
        in_specs=[VMEM],
        out_specs=VMEM,
        out_shape=jax.ShapeDtypeStruct((8, LANES), f32),
        name="sums",
    )(in_hbm(tiles))


def eye_mask(n):
    rows = lax.broadcasted_iota(jnp.int32, (n, n), 0)
    return rows == lax.broadcasted_iota(jnp.int32, (n, n), 1)


def doubled(left_ref, right_ref, power_ref, total_ref):
    n = power_ref.shape[0]
    power, total = power_ref[...], total_ref[...]
    stack_right(right_ref, power)
    for half, x in enumerate((power, total)):
        pieces = thirds(x)
        for k, (i, _) in enumerate(PAIRS):
            left_ref[half * n : (half + 1) * n, k * n : (k + 1) * n] = pieces[i]
    both = jnp.dot(left_ref[...], right_ref[...], preferred_element_type=f32)
    power_ref[...] = both[:n]
    total_ref[...] = total + both[n:]


def prep_kernel(
    rows, loops_ref, turned_ref, both16_ref, design16_ref, six_ref, direct_ref,
    tall_ref, power_ref, total_ref, left_ref, right_ref,
):
    peers = tall_ref.shape[0] // rows
    n = turned_ref.shape[0]
    for source, base, tall in ((loops_ref, n, None), (turned_ref, 0, design16_ref)):
        for start in range(0, source.shape[0], LANES):
            size = min(LANES, source.shape[0] - start)
            tall_ref[:, :size] = source[start : start + size, :].astype(f32).T
            for r in range(rows):
                some = tall_ref[pl.ds(r, peers, stride=rows), :]
                both16_ref[base + start : base + start + size, r * peers : (r + 1) * peers] = some.T[:size].astype(bf16)
                if tall is not None:
                    tall[r * peers : (r + 1) * peers, start : start + size] = some[:, :size].astype(bf16)
    eye = eye_mask(n)
    turned16 = both16_ref[:n, :]
    gram = jnp.dot(turned16, design16_ref[...], preferred_element_type=f32)
    on_diagonal = jnp.where(eye, gram + ridge_weight, 0.0)
    column = jnp.sum(on_diagonal, axis=1, keepdims=True)
    row = jnp.sum(on_diagonal, axis=0, keepdims=True)
    power_ref[...] = jnp.where(eye, 0.0, -gram) / column
    total_ref[...] = jnp.where(eye, 1.0, 0.0)

    def norm():
        return jnp.max(jnp.sum(power_ref[...], axis=1))

    def double(_):
        doubled(left_ref, right_ref, power_ref, total_ref)
        return norm()

    lax.while_loop(lambda size: size > 3e-8, double, norm())
    pieces = thirds(total_ref[...] / row)
    for k, (i, _) in enumerate(PAIRS):
        six_ref[:, k * n : (k + 1) * n] = pieces[i]
    direct_ref[...] = sum(jnp.dot(p, both16_ref[:n, :], preferred_element_type=f32) for p in reversed(pieces))


def prep(loops, design, rows):
    n, m = loops.shape
    dates = design.shape[1]
    return pl.pallas_call(
        functools.partial(prep_kernel, rows),
        in_specs=[VMEM, VMEM],
        out_specs=[VMEM] * 4,
        out_shape=[
            pltpu.HBM((dates + n, m), bf16),
            pltpu.HBM((m, dates), bf16),
            pltpu.HBM((dates, dates * len(PAIRS)), bf16),
            pltpu.HBM((dates, m), f32),
        ],
        scratch_shapes=[
            pltpu.VMEM((m, LANES), f32),
            pltpu.VMEM((dates, dates), f32),
            pltpu.VMEM((dates, dates), f32),
            pltpu.VMEM((2 * dates, dates * len(PAIRS)), bf16),
            pltpu.VMEM((dates * len(PAIRS), dates), bf16),
        ],
        compiler_params=SMALL,
        name="prep",
    )(loops, design.T)


def lines_of(held_ref, r, parts, peers):
    pitch = held_ref.shape[0] // peers
    return jnp.concatenate(
        [held_ref[pl.ds(r * parts + j, peers, stride=pitch), :] for j in range(parts)], axis=1
    )


def main_kernel(
    parts, rows, peers, held_ref, mine_ref, other_ref, both_hbm, six_hbm, design_hbm, shifts_ref, line_ref, closure_hbm,
    both_ref, six_ref, design_ref, wide_ref, stack_ref, closure_ref, sems,
):
    pairs = ((both_hbm, both_ref), (six_hbm, six_ref), (design_hbm, design_ref))
    copies = [pltpu.make_async_copy(a, b, sems.at[k]) for k, (a, b) in enumerate(pairs)]
    copies[0].start()
    for r in range(rows):
        side_by_side(wide_ref, slice(r * peers, (r + 1) * peers), lines_of(held_ref, r, parts, peers))
    copies[0].wait()
    copies[1].start()
    copies[2].start()
    products = folded(jnp.dot(both_ref[...], wide_ref[...], preferred_element_type=f32), 3)
    dates = shifts_ref.shape[0]
    closure_ref[...] = products[dates:]
    copies.append(pltpu.make_async_copy(closure_ref, closure_hbm.at[0], sems.at[3]))
    copies[3].start()
    stack_right(stack_ref, products[:dates])
    copies[1].wait()
    shifts = jnp.dot(six_ref[...], stack_ref[...], preferred_element_type=f32)
    shifts_ref[...] = shifts
    two = jnp.concatenate(thirds(shifts)[:2], axis=1)
    copies[2].wait()
    model = folded(jnp.dot(design_ref[...], two, preferred_element_type=f32), 2)
    square = 0.0
    for r in range(rows):
        residual = lines_of(held_ref, r, parts, peers) - model[r * peers : (r + 1) * peers]
        square += jnp.sum((residual * residual).reshape(peers // 8, 8, parts * LANES), axis=0)
    lane = lax.broadcasted_iota(jnp.int32, (1, LANES), 1)
    line = jnp.where(lane == 0, jnp.sum(square, keepdims=True), mine_ref[:1] + other_ref[:1])
    line_ref[...] = jnp.broadcast_to(line, line_ref.shape)
    copies[3].wait()


def main_part(c, mine, other, both16, six, design16, parts, rows, peers):
    ifgs, dates = design16.shape
    pixels = parts * LANES
    n = both16.shape[0] - dates
    return pl.pallas_call(
        functools.partial(main_kernel, parts, rows, peers),
        in_specs=[VMEM] * 3 + [HBM] * 3,
        out_specs=[VMEM, VMEM, HBM],
        out_shape=[
            jax.ShapeDtypeStruct((dates, pixels), f32),
            jax.ShapeDtypeStruct((peers, LANES), f32),
            pltpu.HBM((1, n, pixels), f32),
        ],
        scratch_shapes=[
            pltpu.VMEM(both16.shape, bf16),
            pltpu.VMEM(six.shape, bf16),
            pltpu.VMEM(design16.shape, bf16),
            pltpu.VMEM((ifgs, 3 * pixels), bf16),
            pltpu.VMEM((dates * len(PAIRS), pixels), bf16),
            pltpu.VMEM((n, pixels), f32),
            pltpu.SemaphoreType.DMA((4,)),
        ],
        compiler_params=pltpu.CompilerParams(vmem_limit_bytes=28 * 2**20),
        name="main",
    )(c, mine, other, in_hbm(both16), in_hbm(six), in_hbm(design16))


def last_kernel(rows, count, squares, got_ref, direct_ref, shifts_ref, displacement_ref, misfit_ref):
    by_lane = got_ref[...].T
    square = jnp.sum(by_lane[:1], axis=1, keepdims=True)
    misfit_ref[...] = jnp.broadcast_to(jnp.sqrt(square / squares + epsilon), misfit_ref.shape)
    line = jnp.concatenate([by_lane[r + 1 : r + 2] for r in range(rows)], axis=1)
    mean = jnp.sum(direct_ref[...] * line, axis=1, keepdims=True) / count
    displacement_ref[0] = shifts_ref[...] - mean


def last_part(got, direct, shifts, rows, count, squares):
    return pl.pallas_call(
        functools.partial(last_kernel, rows, count, squares),
        in_specs=[VMEM] * 3,
        out_specs=[VMEM] * 2,
        out_shape=[
            jax.ShapeDtypeStruct((1, *shifts.shape), f32),
            jax.ShapeDtypeStruct((1, LANES), f32),
        ],
        compiler_params=SMALL,
        name="last",
    )(got, direct, shifts)


def local(phase, corrections, closure_loops, design):
    slabs = lax.axis_size("slab")
    peers = lax.axis_size(IFG)
    rows, pixels = phase.shape[1:]
    parts = pixels // (peers * LANES)
    lines = (rows, pixels // LANES, LANES)
    tiles = head(phase.reshape(lines), corrections.reshape(lines), parts, 4)
    got = lax.all_to_all(tiles.reshape(peers, 1, -1), IFG, split_axis=0, concat_axis=0, tiled=True)
    got = got.reshape(tiles.shape)
    mine = sums_part(tiles, rows, parts, peers)
    other = lax.ppermute(mine, "slab", [(i, (i + 1) % slabs) for i in range(slabs)])
    both16, design16, six, direct = prep(closure_loops, design, rows)
    shifts, line, closure = main_part(got, mine, other, both16, six, design16, parts, rows, peers)
    totals = lax.all_to_all(line.reshape(peers, 1, LANES), IFG, split_axis=0, concat_axis=0, tiled=True)
    displacement, misfit = last_part(
        totals.reshape(peers, LANES), direct, shifts, rows, slabs * pixels, design.shape[0] * pixels
    )
    return (closure, displacement, misfit[0, :1])


def solution(mesh):
    split = Mesh(
        mesh.devices.reshape(4, 4, 4, 2, mesh.shape["slab"]),
        (*IFG, "slab"),
    )
    in_specs = (P("slab", IFG, None), P("slab", IFG, None), P(), P())
    out_specs = (P("slab", None, IFG), P("slab", None, IFG), P("slab"))
    return jax.shard_map(local, mesh=split, in_specs=in_specs, out_specs=out_specs, check_vma=False)
```
